256 devices in a mesh: node: 32 (over z, y_hi, core), ell: 8 (over y_lo, x).
Axes of the slice: x: 4, y: 4 (y_hi: 2, y_lo: 2; y = y_hi * 2 + y_lo), z: 8, core: 2. Of those that a mesh axis runs over, the one named last changes fastest.
Arguments:
- table_zero: bfloat16 [12288, 6144], P('node', 'ell'), may hold values from -1 to 1
- table_two: bfloat16 [12288, 6144], P('node', 'ell'), may hold values from -1 to 1
- spectrum: bfloat16 [6144], P('ell'), may hold values from -0.078125 to 0.078125
- weights: float32 [12288], P('node'), may hold values from 0.018042196 to 0.18042196
Outputs:
- kernel: float32 [6144, 6144], P('node', 'ell')
The draws below stay inside these ranges and needn't reach their ends.
All inputs are finite; a program needn't handle non-finite values.
Results may differ from the reference program's by a relative error of at most 0.0029.
Values may be sent and summed in bfloat16 or wider, within the bound.
No kernel may reach another device: no remote copies, remote signals or barrier semaphores. Data moves between devices by JAX's collectives and lax.ppermute only.
A program may use at most 128 MiB of HBM per device.

```python
import math
import jax
import jax.numpy as jnp
from jax import lax

L = 6144
NODES = 12288


def block_levels(rng, dims, split, smallest, largest):
    gain, own = 1.0, jax.random.fold_in(rng, 6)
    for dim, shards_of in split:
        heights = jnp.exp(jax.random.uniform(jax.random.fold_in(own, dim), (shards_of,), jnp.float32, smallest / len(split), largest / len(split)))
        gain = gain * jnp.repeat(heights, dims[dim] // shards_of).reshape([-1 if axis == dim else 1 for axis in range(len(dims))])
    return gain


def normal_values(stream_key, extent, deviation, most, split=(), dtype=jnp.bfloat16):
    values = deviation * jax.random.normal(stream_key, extent, jnp.float32)
    if split:
        values = values * block_levels(stream_key, extent, split, -0.22, 0.18)
    return jnp.clip(values, -most, most).astype(dtype)


def setup_inputs(seed: int = 0) -> dict:
    streams_of = jax.random.split(jax.random.key(seed), 5)
    return {
        "table_zero": jnp.clip(jax.random.uniform(streams_of[0], (NODES, L), jnp.float32, -1.0, 1.0) * block_levels(streams_of[0], (NODES, L), ((0, 32), (1, 8)), -0.4, 0.0), -1.0, 1.0).astype(jnp.bfloat16),
        "table_two": jnp.clip(jax.random.uniform(streams_of[1], (NODES, L), jnp.float32, -1.0, 1.0) * block_levels(streams_of[1], (NODES, L), ((0, 32), (1, 8)), -0.4, 0.0), -1.0, 1.0).astype(jnp.bfloat16),
        "spectrum": normal_values(streams_of[2], (L,), L ** -0.5, 0.078125, ((0, 8),)),
        "weights": jnp.clip(jnp.exp(math.log(0.18042196) - 2.3025851 * jax.random.uniform(streams_of[3], (NODES,), jnp.float32) ** block_levels(streams_of[3], (NODES,), ((0, 32),), -0.2, 0.2)), 0.018042196, 0.18042196),
    }


def reference(table_zero, table_two, spectrum, weights):
    xi = jnp.dot(table_zero, spectrum, preferred_element_type=jnp.float32)
    weighted = ((weights * xi)[:, None] * table_zero.astype(jnp.float32)).astype(jnp.bfloat16)
    return lax.dot_general(weighted, table_two, (((0,), (0,)), ((), ())), preferred_element_type=jnp.float32)
```

```python
import jax
import jax.numpy as jnp
from jax import lax
from jax.sharding import Mesh, PartitionSpec as P

BF = jnp.bfloat16
F32 = jnp.float32
SENT = jnp.bfloat16
Z, X, Y = 8, 4, 4


def shift(array, axis, size, by):
    return lax.ppermute(array, axis, [(i, (i + by) % size) for i in range(size)])


def per_device(table_zero, table_two, spectrum, weights):
    nodes, cols = table_zero.shape
    half = cols // 8
    iz, iyl, ix = lax.axis_index("z"), lax.axis_index("yl"), lax.axis_index("x")
    yy = ("yh", "yl")

    flipped = table_zero.T
    pieces = lax.all_to_all(
        flipped.reshape(8, half, nodes), ("yh", "c", "yl"), split_axis=0, concat_axis=0, tiled=True
    )
    share = jnp.dot(table_zero, spectrum, preferred_element_type=F32)
    shares = lax.all_to_all(
        jnp.broadcast_to(share, (32, nodes)), ("yh", "c", "yl", "x"), split_axis=0, concat_axis=0, tiled=True
    )
    xi = shares.reshape(4, 8, nodes).sum(axis=1)
    heft = lax.all_gather(weights, ("yh", "c"), axis=0, tiled=False)
    scale = (heft * xi).reshape(4 * nodes)

    own2 = table_two
    below = shift(own2, yy, Y, 1)
    above = shift(own2, yy, Y, -1)
    mid = nodes // 2
    far = jnp.concatenate([shift(below[:mid], yy, Y, 1), shift(above[mid:], yy, Y, -1)], axis=0)
    mate = jnp.where(iyl == 0, above, below)
    cross = jnp.where(iyl == 0, below, above)
    left = jnp.concatenate([own2, mate], axis=1)
    right = jnp.concatenate([far, cross], axis=1)
    mine = jnp.stack([left, right])
    theirs = shift(mine, "c", 2, 1)

    lower = shift(pieces, "x", X, 1)
    upper = shift(pieces, "x", X, -1)
    across = jnp.concatenate([shift(lower[:4], "x", X, 1), shift(upper[4:], "x", X, -1)], axis=0)
    rel = jnp.stack([pieces, upper, across, lower])
    rel = rel.reshape(4, 4, 2, half, nodes)
    rel = rel.transpose(0, 2, 3, 1, 4).reshape(4, 2, half, 4 * nodes)
    lhs = (scale * rel.astype(F32)).astype(BF)

    iyh, ic = lax.axis_index("yh"), lax.axis_index("c")
    both = jnp.stack([mine, theirs], axis=1)
    both = jnp.where(iyh == 0, both, both[::-1])
    both = jnp.where(ic == 0, both, both[:, ::-1])
    rhs = both.reshape(4 * nodes, 2 * cols)

    def rows_for(delta):
        dest = (iz + delta) % Z
        return lax.dynamic_slice(
            lhs, ((dest - ix) % X, dest // X, 0, 0), (1, 1, half, 4 * nodes)
        )[0, 0]

    order = (4, -3, 3, -2, 2, -1, 1, 0)
    left_rows = jnp.concatenate([rows_for(d) for d in order], axis=0)
    product = jnp.dot(left_rows, rhs, preferred_element_type=F32)
    part = {d: product[i * half : (i + 1) * half] for i, d in enumerate(order)}

    down = shift(part[4][:, :cols].astype(SENT), "z", Z, -1)
    up = shift(part[4][:, cols:].astype(SENT), "z", Z, 1)
    zero = jnp.zeros((half, cols), F32)
    down = jnp.concatenate([down.astype(F32), zero], axis=1)
    up = jnp.concatenate([zero, up.astype(F32)], axis=1)
    for step in (3, 2, 1):
        down = shift((down + part[-step]).astype(SENT), "z", Z, -1).astype(F32)
        up = shift((up + part[step]).astype(SENT), "z", Z, 1).astype(F32)
    total = part[0] + down + up
    keep, give = total[:, :cols], total[:, cols:]
    got = shift(give, "yl", 2, 1)
    return jnp.where(
        iyl == 0, jnp.concatenate([keep, got], axis=0), jnp.concatenate([got, keep], axis=0)
    )


def solution(mesh):
    fine = Mesh(mesh.devices.reshape(8, 2, 2, 2, 4), ("z", "yh", "c", "yl", "x"))
    node, ell = ("z", "yh", "c"), ("yl", "x")
    placed = (P(node, ell), P(node, ell), P(ell), P(node))
    return jax.shard_map(
        per_device, mesh=fine, in_specs=placed, out_specs=P(node, ell), check_vma=False
    )
```

```python
import jax
import jax.numpy as jnp
from jax import lax
from jax.experimental import pallas as pl
from jax.experimental.pallas import tpu as pltpu
from jax.sharding import Mesh, PartitionSpec as P

BF = jnp.bfloat16
F32 = jnp.float32
SENT = jnp.bfloat16
Z, X, Y = 8, 4, 4
ORDER = (4, -3, 3, -2, 2, -1, 1, 0)
TILE = 256


def shift(array, axis, size, by):
    return lax.ppermute(array, axis, [(i, (i + by) % size) for i in range(size)])


def product_kernel(
    at, scale, own, upper, lower, far_a, far_b,
    two, below, above, opp_a, opp_b, two_c, below_c, above_c, opp_c, first_down, first_up, out, lhs, rhs,
):
    nodes = own.shape[2]
    cols = two.shape[1]
    ix, iz, here, b_yh, a_yh, ic = at[0], at[1], at[2], at[3], at[4], at[5]
    for core, parts in ((ic, (two, below, above)), (1 - ic, (two_c, below_c, above_c))):
        rhs[2 * here + core, :, :cols] = parts[0][...]
        rhs[2 * b_yh + core, :, cols:] = parts[1][...]
        rhs[2 * a_yh + core, :, cols:] = parts[2][...]
    mid = nodes // 2
    rhs[2 * (1 - here) + ic, :mid, :cols] = opp_a[...]
    rhs[2 * (1 - here) + ic, mid:, :cols] = opp_b[...]
    rhs[2 * (1 - here) + 1 - ic, :, :cols] = opp_c[...]
    for xrel in range(4):
        for late in range(2):
            dest = late * 4 + lax.rem(ix + xrel, 4)
            delta = lax.rem(dest - iz + 8, 8)
            near = jnp.minimum(delta, 8 - delta)
            slot = jnp.minimum(8 - 2 * near - (delta > 4).astype(jnp.int32), 7)
            for k in range(4):
                if xrel == 0:
                    block = own[2 * k + late]
                elif xrel == 1:
                    block = upper[2 * k + late]
                elif xrel == 3:
                    block = lower[2 * k + late]
                elif k < 2:
                    block = far_a[2 * k + late]
                else:
                    block = far_b[2 * (k - 2) + late]
                weighted = scale[k : k + 1, :] * block.astype(F32)
                lhs[slot, :, k * nodes : (k + 1) * nodes] = weighted.astype(BF)
    left = lhs[...].reshape(-1, 4 * nodes)

    rows = own.shape[1]
    for first, base in ((first_down, 0), (first_up, cols)):

        @pl.loop(0, cols // TILE)
        def _(n):
            inner = pl.ds(pl.multiple_of(n * TILE, TILE), TILE)
            outer = pl.ds(pl.multiple_of(base + n * TILE, TILE), TILE)
            right = rhs[:, :, outer].reshape(4 * nodes, TILE)
            result = jnp.dot(left, right, preferred_element_type=F32)
            first[:, inner] = result[:rows].astype(SENT)
            out[:, outer] = result[rows:]


def per_device(table_zero, table_two, spectrum, weights):
    nodes, cols = table_zero.shape
    half = cols // 8
    iz, iyl, ix = lax.axis_index("z"), lax.axis_index("yl"), lax.axis_index("x")
    iyh, ic = lax.axis_index("yh"), lax.axis_index("c")
    yy = ("yh", "yl")

    flipped = table_zero.T
    pieces = lax.all_to_all(
        flipped.reshape(8, half, nodes), ("yh", "c", "yl"), split_axis=0, concat_axis=0, tiled=True
    )
    share = weights * jnp.dot(table_zero, spectrum, preferred_element_type=F32)
    pieces, share = lax.optimization_barrier((pieces, share))
    shares = lax.all_to_all(
        jnp.broadcast_to(share, (32, nodes)), ("yh", "c", "yl", "x"), split_axis=0, concat_axis=0, tiled=True
    )
    scale = shares.reshape(4, 8, nodes).sum(axis=1)

    mid = nodes // 2
    below = shift(table_two, yy, Y, 1)
    above = shift(table_two, yy, Y, -1)
    two_c = shift(table_two, "c", 2, 1)
    opp_a = shift(below[:mid], yy, Y, 1)
    opp_b = shift(above[mid:], yy, Y, -1)
    below_c = shift(below, "c", 2, 1)
    above_c = shift(above, "c", 2, 1)
    opp_c = shift(jnp.concatenate([opp_a, opp_b], axis=0), "c", 2, 1)

    lower = shift(pieces, "x", X, 1)
    upper = shift(pieces, "x", X, -1)
    far_a = shift(lower[:4], "x", X, 1)
    far_b = shift(upper[4:], "x", X, -1)

    at = jnp.stack(
        [ix, iz, iyh, jnp.where(iyl == 0, 1 - iyh, iyh), jnp.where(iyl == 0, iyh, 1 - iyh), ic]
    ).astype(jnp.int32)
    vmem = pl.BlockSpec(memory_space=pltpu.VMEM)
    down, up, product = pl.pallas_call(
        product_kernel,
        out_shape=(
            jax.ShapeDtypeStruct((half, cols), SENT),
            jax.ShapeDtypeStruct((half, cols), SENT),
            jax.ShapeDtypeStruct((7 * half, 2 * cols), F32),
        ),
        in_specs=[pl.BlockSpec(memory_space=pltpu.SMEM)] + [vmem] * 15,
        out_specs=(vmem, vmem, vmem),
        scratch_shapes=[
            pltpu.VMEM((8, half, 4 * nodes), BF),
            pltpu.VMEM((4, nodes, 2 * cols), BF),
        ],
        compiler_params=pltpu.CompilerParams(vmem_limit_bytes=32 * 2**20),
        cost_estimate=pl.CostEstimate(
            flops=2 * 8 * half * 2 * cols * 4 * nodes, bytes_accessed=12 * 2**20, transcendentals=0
        ),
    )(
        at, scale, pieces, upper, lower, far_a, far_b,
        table_two, below, above, opp_a, opp_b, two_c, below_c, above_c, opp_c,
    )
    part = {d: product[i * half : (i + 1) * half] for i, d in enumerate(ORDER[1:])}

    down = shift(down, "z", Z, -1)
    up = shift(up, "z", Z, 1)
    zero = jnp.zeros((half, cols), F32)
    down = jnp.concatenate([down.astype(F32), zero], axis=1)
    up = jnp.concatenate([zero, up.astype(F32)], axis=1)
    for step in (3, 2, 1):
        down = shift((down + part[-step]).astype(SENT), "z", Z, -1).astype(F32)
        up = shift((up + part[step]).astype(SENT), "z", Z, 1).astype(F32)
    total = part[0] + down + up
    keep, give = total[:, :cols], total[:, cols:]
    got = shift(give, "yl", 2, 1)
    return jnp.where(
        iyl == 0, jnp.concatenate([keep, got], axis=0), jnp.concatenate([got, keep], axis=0)
    )


def solution(mesh):
    fine = Mesh(mesh.devices.reshape(8, 2, 2, 2, 4), ("z", "yh", "c", "yl", "x"))
    node, ell = ("z", "yh", "c"), ("yl", "x")
    placed = (P(node, ell), P(node, ell), P(ell), P(node))
    return jax.shard_map(
        per_device, mesh=fine, in_specs=placed, out_specs=P(node, ell), check_vma=False
    )
```
